128 devices in a mesh: pair: 8 (over x, core), row: 16 (over z, y).
Axes of the slice: x: 4, y: 4, z: 4, core: 2. Of those that a mesh axis runs over, the one named last changes fastest.
Arguments:
- descriptors: bfloat16 [64, 2048, 256], P('pair', 'row'), parts along dimension 0, may hold values from -8 to 8
- counts: int32 [64], P('pair'), parts along dimension 0, may hold values from 512 to 2048
- pairs: int32 [32, 2], P('pair'), parts along dimension 0, may hold values from 0 to 7, as said below
- bin_score: float32 [1], replicated, may hold values from 0.5 to 2
Outputs:
- log_match: float32 [32, 2048, 2048], P('pair', 'row'), parts along dimension 0
- row_bins: float32 [32, 2048], P('pair', 'row'), parts along dimension 0
- col_bins: float32 [32, 2048], P('pair'), parts along dimension 0
The draws below stay inside these ranges and needn't reach their ends.
There are 8 independent parts, one for each index of `pair`. The reference program is written for one: setup_inputs(seed, part) draws one part's arguments, and reference() takes and returns one part's arrays. A program takes and returns all parts, laid end to end along the dimension named above; an argument that names none is the same for every part. Nothing has to cross between parts.
Inputs may be any that keep to these rules, and one draw needn't show every extreme that they name: Image k's keypoints are its first counts[k] slots. `pairs`: the two images of a pair differ.
All inputs are finite; a program needn't handle non-finite values.
Results may differ from the reference program's by a relative error of at most 0.0003.
Values may be sent and summed in bfloat16 or wider, within the bound.
No kernel may reach another device: no remote copies, remote signals or barrier semaphores. Data moves between devices by JAX's collectives and lax.ppermute only.
A program may use at most 64 MiB of HBM per device.

```python
import jax
import jax.numpy as jnp
from jax import lax

PAIRS = 4
IMAGES = 8
KP = 2048
D = 256
ITERS = 10


def draw_descriptors(key, part):
    values = 2.0 * jax.random.truncated_normal(jax.random.fold_in(key, 5), -4.0, 4.0, (IMAGES, KP, D), jnp.float32)
    return values.astype(jnp.bfloat16)


def draw_pairs(key, part):
    first_image = jax.random.randint(jax.random.fold_in(key, 1), (PAIRS,), 0, IMAGES)
    stride = jax.random.randint(jax.random.fold_in(key, 2), (PAIRS,), 1, IMAGES)
    second_image = (first_image + stride) % IMAGES
    return jnp.stack([first_image, second_image], axis=1).astype(jnp.int32)


def set_ends(entries, key, least, largest):
    spot = [jax.random.randint(jax.random.fold_in(key, axis), (), 0, length) for axis, length in enumerate(entries.shape)]
    longest = entries.shape.index(max(entries.shape))
    neighbour = spot[:longest] + [(spot[longest] + 1) % entries.shape[longest]] + spot[longest + 1:]
    return entries.at[tuple(spot)].set(least).at[tuple(neighbour)].set(largest)


def setup_inputs(seed: int = 0, part: int = 0) -> dict:
    keys = jax.random.split(jax.random.key(seed), 5)
    part_splits = jax.random.split(jax.random.fold_in(keys[4], part), 5)
    descriptors = draw_descriptors(jax.random.fold_in(jax.random.fold_in(keys[4], part), 71), part)
    counts = set_ends(jax.random.randint(part_splits[1], (IMAGES,), KP // 4, KP + 1), jax.random.fold_in(part_splits[1], 1), KP // 4, KP).astype(jnp.int32)
    pairs = draw_pairs(jax.random.fold_in(jax.random.fold_in(keys[4], part), 71), part)
    bin_score = jnp.clip(jax.random.uniform(keys[3], (1,), jnp.float32, 0.5, 2.0), 0.5, 2.0)
    return dict(descriptors=descriptors, counts=counts, pairs=pairs, bin_score=bin_score)


NEG = -1.0e30


def masked_lse(values, kept, reduce_dim):
    held = jnp.where(kept, values, NEG)
    ceiling = jnp.max(held, axis=reduce_dim, keepdims=True)
    summed = jnp.sum(jnp.where(kept, jnp.exp(held - ceiling), 0.0), axis=reduce_dim, keepdims=True)
    return jnp.squeeze(ceiling + jnp.log(summed), reduce_dim)


def reference(descriptors, counts, pairs, bin_score):
    bin_value = bin_score[0]
    row_images = descriptors[pairs[:, 0]]
    col_images = descriptors[pairs[:, 1]]
    row_counts = counts[pairs[:, 0]]
    col_counts = counts[pairs[:, 1]]

    def one_pair(operands):
        row_desc, col_desc, n_rows, n_cols = operands
        scores = jnp.dot(row_desc, col_desc.T, preferred_element_type=jnp.float32) * (D ** -0.5)
        side_line = jnp.zeros((KP, 1), jnp.float32) + bin_value
        upper = jnp.concatenate([scores, side_line], axis=1)
        bin_line = jnp.zeros((1, KP + 1), jnp.float32) + bin_value
        couplings = jnp.concatenate([upper, bin_line], axis=0)
        cell_index = jnp.arange(KP + 1, dtype=jnp.int32)
        row_kept = (cell_index < n_rows) | (cell_index == KP)
        col_kept = (cell_index < n_cols) | (cell_index == KP)
        row_count = n_rows.astype(jnp.float32)
        col_count = n_cols.astype(jnp.float32)
        log_norm = -jnp.log(row_count + col_count)
        log_mu = jnp.where(cell_index == KP, jnp.log(col_count) + log_norm, log_norm)
        log_nu = jnp.where(cell_index == KP, jnp.log(row_count) + log_norm, log_norm)
        row_pot = jnp.zeros((KP + 1,), jnp.float32)
        col_pot = jnp.zeros((KP + 1,), jnp.float32)
        for sweep_index in range(ITERS):
            row_pot = log_mu - masked_lse(couplings + col_pot[None, :], col_kept[None, :], 1)
            col_pot = log_nu - masked_lse(couplings + row_pot[:, None], row_kept[:, None], 0)
        assign = couplings + row_pot[:, None] + col_pot[None, :] - log_norm
        assign = jnp.where(row_kept[:, None] & col_kept[None, :], assign, 0.0)
        return assign[:KP, :KP], assign[:KP, KP], assign[KP, :KP]

    log_match, row_bins, col_bins = lax.map(one_pair, (row_images, col_images, row_counts, col_counts))
    return (log_match, row_bins, col_bins)
```

```python
import functools

import jax
import jax.numpy as jnp
from jax import lax
from jax.experimental import pallas as pl
from jax.experimental.pallas import tpu as pltpu
from jax.sharding import Mesh
from jax.sharding import PartitionSpec as P

ITERS = 10
KP = 2048
D = 256
BLK = 128
NBLK = KP // BLK
NCH = KP // 128
BIAS = 40.0
AXES = ("pair", "row_0", "row_1")


def tree_sum(terms):
    while len(terms) > 1:
        pairs = [terms[k] + terms[k + 1] for k in range(0, len(terms) - 1, 2)]
        terms = pairs + ([terms[-1]] if len(terms) % 2 else [])
    return terms[0]


def sinkhorn_kernel(
    meta, counts, pairs, bins, x0, x1, x2, x3, out, rows, cols, kern, part, scale_a, peak, scale_b, sems
):
    own = meta[16]
    n_rows = counts[pairs[own, 0]]
    n_cols = counts[pairs[own, 1]]
    alpha = bins[0]
    copies = []
    for k, x in enumerate((x0, x1, x2, x3)):
        for t in range(4):
            spot = pl.ds(pl.multiple_of(meta[4 * k + t] * BLK, BLK), BLK)
            for side, target in ((1, cols), (0, rows)):
                copy = pltpu.make_async_copy(x.at[t, side], target.at[spot], sems.at[k, t, side])
                copy.start()
                copies.append(copy)
    for copy in copies:
        copy.wait()
    lanes = lax.broadcasted_iota(jnp.int32, (1, 128), 1)
    blocks = (n_rows + BLK - 1) // BLK

    for c in range(NBLK):
        spot = pl.ds(c * BLK, BLK)
        place = c * BLK + lax.broadcasted_iota(jnp.int32, (BLK, D), 0)
        kept = jnp.where(place < n_cols, 1.0, 0.0)
        cols[spot, :] = (cols[spot, :].astype(jnp.float32) * kept).astype(jnp.bfloat16)

    def scores_of(r):
        spot = pl.ds(pl.multiple_of(r * BLK, BLK), BLK)
        left = rows[spot, :] * jnp.bfloat16(0.0625)
        tops = []
        for c in range(KP // 256):
            tile = lax.dot_general(
                left,
                cols[pl.ds(c * 256, 256), :],
                (((1,), (1,)), ((), ())),
                preferred_element_type=jnp.float32,
            )
            kern[spot, pl.ds(c * 256, 256)] = tile
            tops += [tile[:, :128], tile[:, 128:]]
        while len(tops) > 1:
            tops = [jnp.maximum(tops[k], tops[k + 1]) for k in range(0, len(tops), 2)]
        peak[spot, :] = tops[0]

    def exps_of(r):
        spot = pl.ds(pl.multiple_of(r * BLK, BLK), BLK)
        top = jnp.maximum(jnp.max(peak[spot, :], axis=1, keepdims=True), alpha)
        drop = jnp.broadcast_to(top - BIAS, (BLK, 128))
        peak[spot, :] = drop
        for c in range(NCH):
            ch = pl.ds(c * 128, 128)
            kern[spot, ch] = jnp.exp(kern[spot, ch] - drop)
        kern[spot, pl.ds(KP, 128)] = jnp.where(lanes == 0, jnp.exp(alpha - drop), 0.0)

    scores_of(0)

    @pl.loop(1, blocks)
    def _(r):
        exps_of(r - 1)
        scores_of(r)

    exps_of(blocks - 1)

    row_count = jnp.full((1, 128), n_rows.astype(jnp.float32))
    col_count = jnp.full((1, 128), n_cols.astype(jnp.float32))
    mu = 1.0 / (row_count + col_count)
    mu_bin = col_count * mu
    nu_bin = row_count * mu

    for c in range(NCH):
        scale_b[:, pl.ds(c * 128, 128)] = jnp.broadcast_to(
            jnp.where(lanes + c * 128 < n_cols, 1.0, 0.0), (8, 128)
        )
    scale_b[:, pl.ds(KP, 128)] = jnp.broadcast_to(jnp.where(lanes == 0, 1.0, 0.0), (8, 128))

    def sums(r, b):
        base = pl.multiple_of(r * BLK, BLK)
        for g in range(BLK // 8):
            spot = pl.ds(base + 8 * g, 8)
            part[spot, :] = tree_sum(
                [kern[spot, pl.ds(c * 128, 128)] * b[c] for c in range(NCH + 1)]
            )

    def scales(r):
        base = pl.multiple_of(r * BLK, BLK)
        spot = pl.ds(base, BLK)
        total = jnp.sum(part[spot, :], axis=1, keepdims=True)
        place = base + lax.broadcasted_iota(jnp.int32, (BLK, 128), 0)
        scale_a[spot, :] = jnp.where(
            place < n_rows, mu / jnp.broadcast_to(total, (BLK, 128)), 0.0
        )

    def gathers(r, acc):
        base = pl.multiple_of(r * BLK, BLK)
        acc = list(acc)
        for g in range(BLK // 8):
            spot = pl.ds(base + 8 * g, 8)
            a = scale_a[spot, :]
            for c in range(NCH + 1):
                acc[c] = acc[c] + kern[spot, pl.ds(c * 128, 128)] * a
        return tuple(acc)

    def sweep(_, bin_line):
        b = [scale_b[:, pl.ds(c * 128, 128)] for c in range(NCH + 1)]
        whole = jnp.sum(tree_sum(b), axis=1, keepdims=True)[:1]
        bin_line = mu_bin / jnp.broadcast_to(whole, (1, 128))
        sums(0, b)
        sums(1, b)
        scales(0)

        def body(r, acc):
            scales(r - 1)
            acc = gathers(r - 2, acc)
            sums(r, b)
            return acc

        acc = tuple(jnp.zeros((8, 128), jnp.float32) for _ in range(NCH + 1))
        acc = lax.fori_loop(2, blocks, body, acc)
        scales(blocks - 1)
        acc = gathers(blocks - 2, acc)
        acc = gathers(blocks - 1, acc)
        for c in range(NCH + 1):
            total = jnp.sum(acc[c], axis=0, keepdims=True) + bin_line
            if c < NCH:
                fresh = jnp.where(lanes + c * 128 < n_cols, mu / total, 0.0)
            else:
                fresh = jnp.where(lanes == 0, nu_bin / total, 0.0)
            scale_b[:, pl.ds(c * 128, 128)] = jnp.broadcast_to(fresh, (8, 128))
        return bin_line

    bin_line = lax.fori_loop(0, ITERS, sweep, jnp.zeros((1, 128), jnp.float32))

    out[...] = jnp.zeros_like(out)
    diagonal = lax.broadcasted_iota(jnp.int32, (BLK, 128), 0) == lax.broadcasted_iota(
        jnp.int32, (BLK, 128), 1
    )

    @pl.loop(0, blocks)
    def _(r):
        spot = pl.ds(pl.multiple_of(r * BLK, BLK), BLK)
        pot = jnp.log(scale_a[spot, :]) - peak[spot, :]
        out[pl.ds(r, 1), :] = jnp.sum(jnp.where(diagonal, pot, 0.0), axis=0, keepdims=True)

    for c in range(NCH):
        out[NBLK + c : NBLK + c + 1, :] = jnp.log(scale_b[0:1, pl.ds(c * 128, 128)])
    out[32:33, :] = jnp.log(bin_line) - alpha
    bin_pot = jnp.where(lanes == 0, jnp.log(scale_b[0:1, pl.ds(KP, 128)]), 0.0)
    out[33:34, :] = jnp.broadcast_to(jnp.sum(bin_pot, axis=1, keepdims=True), (1, 128))


def finish_kernel(
    meta, counts, pairs, bins, desc, c0, c1, c2, c3, p0, p1, p2, p3,
    match, row_bins, col_bins, cols, block, edge, in_sems, out_sems,
):
    alpha = bins[0]
    mine = meta[68]
    loads = []
    for m, c in enumerate((c0, c1, c2, c3)):
        copy = pltpu.make_async_copy(c, cols.at[m], in_sems.at[m])
        copy.start()
        loads.append(copy)
    lanes = lax.broadcasted_iota(jnp.int32, (1, 128), 1)
    row_id = lax.broadcasted_iota(jnp.int32, (BLK, 128), 0)
    diagonal = row_id == lax.broadcasted_iota(jnp.int32, (BLK, 128), 1)
    quarter = lax.broadcasted_iota(jnp.int32, (4, 128), 0)
    row_bins[...] = jnp.zeros_like(row_bins)
    stores = []
    for m, pay in enumerate((p0, p1, p2, p3)):
        p = meta[64 + m]
        n_rows = counts[pairs[p, 0]]
        n_cols = counts[pairs[p, 1]]
        both = n_rows.astype(jnp.float32) + n_cols.astype(jnp.float32)
        norm = -jnp.log(jnp.full((1, 128), both))
        line = pay[pl.ds(mine, 1), :]
        pot = jnp.sum(
            jnp.where(diagonal, jnp.broadcast_to(line, (BLK, 128)), 0.0), axis=1, keepdims=True
        )
        pot = jnp.broadcast_to(pot, (BLK, 128))
        row_kept = mine * BLK + row_id < n_rows
        side = jnp.where(mine * BLK + lanes < n_rows, alpha + line + pay[33:34, :] - norm, 0.0)
        row_bins[...] = jnp.where(quarter == p, side, row_bins[...])
        left = desc[pairs[p, 0]] * jnp.bfloat16(0.0625)
        loads[m].wait()
        for k in range(4):
            for t in range(4):
                at = meta[16 * m + 4 * k + t]
                col_pot = pay[pl.ds(NBLK + at, 1), :]
                col_kept = at * BLK + lanes < n_cols
                tile = lax.dot_general(
                    left, cols[m, k, t], (((1,), (1,)), ((), ())), preferred_element_type=jnp.float32
                )
                tile = tile + pot + col_pot - norm
                spot = pl.ds(pl.multiple_of(at * BLK, BLK), BLK)
                block[m, :, spot] = jnp.where(row_kept & col_kept, tile, 0.0)
                edge[m, :, spot] = jnp.where(
                    col_kept, alpha + pay[32:33, :] + col_pot - norm, 0.0
                )
        copy = pltpu.make_async_copy(block.at[m], match.at[p], out_sems.at[m])
        copy.start()
        stores.append(copy)
    for c in range(NCH):
        spot = pl.ds(c * 128, 128)
        line = jnp.zeros((4, 128), jnp.float32)
        for m in range(4):
            line = jnp.where(quarter == meta[64 + m], edge[m, :, spot], line)
        col_bins[:, spot] = line
    for copy in stores:
        copy.wait()


SMEM = functools.partial(pl.BlockSpec, memory_space=pltpu.SMEM)
VMEM = functools.partial(pl.BlockSpec, memory_space=pltpu.VMEM)
ANY = functools.partial(pl.BlockSpec, memory_space=pl.ANY)


def run_sinkhorn(meta, counts, pairs, bins, xs):
    f32 = jnp.float32
    return pl.pallas_call(
        sinkhorn_kernel,
        out_shape=jax.ShapeDtypeStruct((40, 128), f32),
        in_specs=[SMEM()] * 4 + [ANY()] * 4,
        out_specs=VMEM(),
        scratch_shapes=[
            pltpu.VMEM((KP, D), jnp.bfloat16),
            pltpu.VMEM((KP, D), jnp.bfloat16),
            pltpu.VMEM((KP, KP + 128), f32),
            pltpu.VMEM((KP, 128), f32),
            pltpu.VMEM((KP, 128), f32),
            pltpu.VMEM((KP, 128), f32),
            pltpu.VMEM((8, KP + 128), f32),
            pltpu.SemaphoreType.DMA((4, 4, 2)),
        ],
        compiler_params=pltpu.CompilerParams(vmem_limit_bytes=40 * 1024 * 1024),
        cost_estimate=pl.CostEstimate(
            flops=200_000_000_000, bytes_accessed=2 << 20, transcendentals=0
        ),
        name="sinkhorn",
    )(meta, counts, pairs, bins, *xs)


def run_finish(meta, counts, pairs, bins, desc, cs, pays):
    f32 = jnp.float32
    return pl.pallas_call(
        finish_kernel,
        out_shape=(
            jax.ShapeDtypeStruct((4, BLK, KP), f32),
            jax.ShapeDtypeStruct((4, BLK), f32),
            jax.ShapeDtypeStruct((4, KP), f32),
        ),
        in_specs=[SMEM()] * 4 + [VMEM()] + [ANY()] * 4 + [VMEM()] * 4,
        out_specs=(ANY(), VMEM(), VMEM()),
        scratch_shapes=[
            pltpu.VMEM((4, 4, 4, BLK, D), jnp.bfloat16),
            pltpu.VMEM((4, BLK, KP), f32),
            pltpu.VMEM((4, 1, KP), f32),
            pltpu.SemaphoreType.DMA((4,)),
            pltpu.SemaphoreType.DMA((4,)),
        ],
        compiler_params=pltpu.CompilerParams(vmem_limit_bytes=24 * 1024 * 1024),
        name="finish",
    )(meta, counts, pairs, bins, desc, *cs, *pays)


def shifts(groups, along_b):
    def perm(k):
        moves = []
        for g in range(groups):
            for i in range(4):
                for j in range(4):
                    on_row_1 = (g % 2 == 0) == along_b
                    to = (i, (j + k) % 4) if on_row_1 else ((i + k) % 4, j)
                    moves.append((g * 16 + i * 4 + j, g * 16 + to[0] * 4 + to[1]))
        return moves

    return perm


def on_device(descriptors, counts, pairs, bin_score):
    groups = lax.axis_size("pair")
    even = lax.axis_index("pair") % 2 == 0
    i, j = lax.axis_index("row_0"), lax.axis_index("row_1")
    a, b = jnp.where(even, i, j), jnp.where(even, j, i)
    by_b, by_a = shifts(groups, True), shifts(groups, False)

    def block_of(a_at, b_at):
        return jnp.where(even, a_at * 4 + b_at, b_at * 4 + a_at)

    four = jnp.arange(4, dtype=jnp.int32)
    a_at = ((a - four) % 4)[None, :, None]
    b_at = ((b - four[:, None] - four[None, :]) % 4)[:, None, :]
    where = block_of(a_at, b_at).reshape(-1)
    owner = (b - four) % 4
    meta = jnp.concatenate([where, owner, (i * 4 + j)[None]]).astype(jnp.int32)
    meta_own = jnp.concatenate([where[:16], owner[:1]]).astype(jnp.int32)

    def blocks_for(k):
        return descriptors[pairs[(b + k) % 4]]

    first = [blocks_for(0)]
    for k in (1, 2, 3):
        first.append(lax.ppermute(blocks_for(k), AXES, by_b(k)))
    x0 = jnp.stack(first)
    xs = [x0] + [lax.ppermute(x0, AXES, by_a(k)) for k in (1, 2, 3)]
    c0 = jnp.stack([x[:, 1] for x in xs])
    cs = [c0] + [lax.ppermute(c0, AXES, by_b(k)) for k in (1, 2, 3)]
    pay = run_sinkhorn(meta_own, counts, pairs, bin_score, xs)
    pays = [pay] + [lax.ppermute(pay, AXES, by_b(k)) for k in (1, 2, 3)]
    return run_finish(meta, counts, pairs, bin_score, descriptors, cs, pays)


def solution(mesh):
    finer = Mesh(mesh.devices.reshape(mesh.shape["pair"], 4, 4), AXES)
    rows = ("row_0", "row_1")
    in_specs = (P("pair", rows, None), P("pair"), P("pair", None), P())
    out_specs = (P("pair", rows, None), P("pair", rows), P("pair", None))
    return jax.shard_map(
        on_device, mesh=finer, in_specs=in_specs, out_specs=out_specs, check_vma=False
    )
```

```python
import functools

import jax
import jax.numpy as jnp
from jax import lax
from jax.experimental import pallas as pl
from jax.experimental.pallas import tpu as pltpu
from jax.sharding import Mesh
from jax.sharding import PartitionSpec as P

ITERS = 10
KP = 2048
D = 256
BLK = 128
NBLK = KP // BLK
NCH = KP // 128
BIAS = 40.0
BIG = 256
SHARE = 8
AXES = ("pair", "row_0", "row_1")


def tree_sum(terms):
    while len(terms) > 1:
        pairs = [terms[k] + terms[k + 1] for k in range(0, len(terms) - 1, 2)]
        terms = pairs + ([terms[-1]] if len(terms) % 2 else [])
    return terms[0]


def sinkhorn_kernel(
    params, bins, x0, x1, x2, x3, out,
    kern, raw_0, raw_1, rows, cols, part, peak, wide_a, wide_mu, bin_hot, scale_b, share_b, sems,
):
    n_rows = params[4]
    n_cols = params[8]
    alpha = bins[0]
    copies = []
    for k, x in enumerate((x0, x1, x2, x3)):
        for t in range(4):
            spot = pl.ds(pl.multiple_of(block_at(params, 0, k, t) * BLK, BLK), BLK)
            for side, target in ((1, cols), (0, rows)):
                copy = pltpu.make_async_copy(x.at[t, side], target.at[spot], sems.at[k, t, side])
                copy.start()
                copies.append(copy)
    lanes = lax.broadcasted_iota(jnp.int32, (1, 128), 1)
    row_count = jnp.full((8, 128), n_rows.astype(jnp.float32))
    col_count = jnp.full((8, 128), n_cols.astype(jnp.float32))
    mu = 1.0 / (row_count + col_count)
    mu_bin = col_count * mu
    nu_bin = row_count * mu
    for c in range(NCH):
        kept = jnp.broadcast_to(lanes + c * 128 < n_cols, (8, 128))
        scale_b[:, pl.ds(c * 128, 128)] = jnp.where(kept, 1.0, 0.0)
        share_b[:, pl.ds(c * 128, 128)] = jnp.where(kept, mu, 0.0)
    out[...] = jnp.zeros_like(out)
    pair_rows = 2 * BIG
    steps = (n_rows + pair_rows - 1) // pair_rows
    for copy in copies:
        copy.wait()

    @pl.loop(0, NBLK)
    def _(c):
        spot = pl.ds(pl.multiple_of(c * BLK, BLK), BLK)
        place = c * BLK + lax.broadcasted_iota(jnp.int32, (BLK, D), 0)
        kept = jnp.where(place < n_cols, 1.0, 0.0)
        cols[spot, :] = (cols[spot, :].astype(jnp.float32) * kept).astype(jnp.bfloat16)
        for g in range(0, BLK, 8):
            at = pl.ds(pl.multiple_of(c * BLK + g, 8), 8)
            row = c * BLK + g + lax.broadcasted_iota(jnp.int32, (8, 128), 0)
            wide_mu[at, :] = jnp.where(row < n_rows, mu, 0.0)

    def block(r):
        return pl.multiple_of(r * BIG, BIG)

    def scores_of(r, raw):
        left = rows[pl.ds(block(r), BIG), :] * jnp.bfloat16(0.0625)
        for c in range(NCH // 2):
            raw[:, pl.ds(c * 256, 256)] = lax.dot_general(
                left,
                cols[pl.ds(c * 256, 256), :],
                (((1,), (1,)), ((), ())),
                preferred_element_type=jnp.float32,
            )

    def exps_of(r, raw):
        base = block(r)
        for g in range(0, BIG, 8):
            at, near = pl.ds(base + g, 8), pl.ds(g, 8)
            tops = [raw[near, pl.ds(c * 128, 128)] for c in range(NCH)]
            while len(tops) > 1:
                tops = [jnp.maximum(tops[k], tops[k + 1]) for k in range(0, len(tops), 2)]
            drop = jnp.maximum(jnp.max(tops[0], axis=1, keepdims=True), alpha) - BIAS
            peak[at, :] = jnp.broadcast_to(drop, (8, 128))
        for g in range(0, BIG, 8):
            at, near = pl.ds(base + g, 8), pl.ds(g, 8)
            drop = peak[at, :]
            for c in range(NCH):
                ch = pl.ds(c * 128, 128)
                kern[at, ch] = jnp.exp(raw[near, ch] - drop)
            bin_hot[at, :] = jnp.where(lanes == 0, jnp.exp(alpha - drop), 0.0)

    scores_of(0, raw_0)

    @pl.loop(0, steps - 1)
    def _(m):
        scores_of(2 * m + 1, raw_1)
        exps_of(2 * m, raw_0)
        scores_of(2 * m + 2, raw_0)
        exps_of(2 * m + 1, raw_1)

    scores_of(2 * steps - 1, raw_1)
    exps_of(2 * steps - 2, raw_0)
    exps_of(2 * steps - 1, raw_1)

    def sums(r, bin_b, low):
        base = block(r)
        for q in range(0, BIG // 8, SHARE):
            sets = [pl.ds(base + 8 * (q + g), 8) for g in range(SHARE)]
            acc = [bin_hot[sets[g], :] * bin_b for g in range(SHARE)]
            for c in range(NCH):
                ch = pl.ds(c * 128, 128)
                b = scale_b[:, ch]
                for g in range(SHARE):
                    acc[g] = acc[g] + kern[sets[g], ch] * b
            for g in range(SHARE):
                part[pl.ds(low + 8 * (q + g), 8), :] = acc[g]

    def scales(r, low):
        base = block(r)
        for g in range(0, BIG, 8):
            at = pl.ds(base + g, 8)
            total = jnp.sum(part[pl.ds(low + g, 8), :], axis=1, keepdims=True)
            wide_a[at, :] = wide_mu[at, :] / jnp.broadcast_to(total, (8, 128))

    def gathers(r, acc):
        acc = list(acc)
        base = block(r)
        for g in range(0, BIG, 8):
            at = pl.ds(base + g, 8)
            a = wide_a[at, :]
            for c in range(NCH):
                acc[c] = acc[c] + kern[at, pl.ds(c * 128, 128)] * a
            acc[NCH] = acc[NCH] + bin_hot[at, :] * a
        return tuple(acc)

    def sweep(_, carry):
        bin_b, _ = carry
        whole = tree_sum([scale_b[:, pl.ds(c * 128, 128)] for c in range(NCH)])
        whole = jnp.broadcast_to(jnp.sum(whole, axis=1, keepdims=True), (8, 128))
        bin_line = mu_bin / (whole + bin_b)
        sums(0, bin_b, 0)

        @pl.loop(0, steps - 1)
        def _(m):
            sums(2 * m + 1, bin_b, BIG)
            scales(2 * m, 0)
            sums(2 * m + 2, bin_b, 0)
            scales(2 * m + 1, BIG)

        sums(2 * steps - 1, bin_b, BIG)
        scales(2 * steps - 2, 0)
        scales(2 * steps - 1, BIG)
        zero = jnp.zeros((8, 128), jnp.float32)
        acc = lax.fori_loop(0, 2 * steps, gathers, (zero,) * (NCH + 1))
        for c in range(NCH):
            ch = pl.ds(c * 128, 128)
            total = jnp.broadcast_to(jnp.sum(acc[c], axis=0, keepdims=True), (8, 128))
            scale_b[:, ch] = share_b[:, ch] / (total + bin_line)
        bin_acc = jnp.broadcast_to(jnp.sum(acc[NCH], axis=0, keepdims=True), (8, 128))
        bin_sum = jnp.broadcast_to(jnp.sum(bin_acc, axis=1, keepdims=True), (8, 128))
        return nu_bin / (bin_sum + bin_line), bin_line

    ones = jnp.ones((8, 128), jnp.float32)
    bin_b, bin_line = lax.fori_loop(0, ITERS, sweep, (ones, ones))

    @pl.loop(0, (n_rows + BLK - 1) // BLK)
    def _(r):
        spot = pl.ds(pl.multiple_of(r * BLK, BLK), BLK)
        pot = jnp.log(wide_a[spot, :]) - peak[spot, :]
        out[pl.ds(r, 1), :] = jnp.transpose(pot)[:1]

    for c in range(NCH):
        out[NBLK + c : NBLK + c + 1, :] = jnp.log(scale_b[0:1, pl.ds(c * 128, 128)])
    out[32:33, :] = (jnp.log(bin_line) - alpha)[:1]
    out[33:34, :] = jnp.log(bin_b)[:1]


def block_at(params, m, k, t):
    a = lax.rem(params[0] - k + 4, 4)
    b = lax.rem(params[1] - m - t + 8, 4)
    return jnp.where(params[2] == 1, a * 4 + b, b * 4 + a)


def pick_kernel(index, counts, pairs, desc, s0, s1, s2, s3, params, sems):
    b = index[1]
    copies = []
    for k, target in ((1, s1), (2, s2), (3, s3), (0, s0)):
        p = lax.rem(b + k, 4)
        for side in range(2):
            copy = pltpu.make_async_copy(desc.at[pairs[p, side]], target.at[side], sems.at[k, side])
            copy.start()
            copies.append(copy)
    for c in range(4):
        params[c] = index[c]
    for m in range(4):
        p = lax.rem(b - m + 4, 4)
        params[4 + m] = counts[pairs[p, 0]]
        params[8 + m] = counts[pairs[p, 1]]
        params[12 + m] = pairs[p, 0]
        params[16 + m] = p
    for copy in copies:
        copy.wait()


def score_kernel(params, desc, c0, c1, c2, c3, scores, cols, sems):
    loads = []
    for m, c in enumerate((c0, c1, c2, c3)):
        copy = pltpu.make_async_copy(c, cols.at[m], sems.at[m])
        copy.start()
        loads.append(copy)
    for m in range(4):
        left = desc[params[12 + m]] * jnp.bfloat16(0.0625)
        loads[m].wait()
        for k in range(4):
            for t in range(4):
                spot = pl.ds(pl.multiple_of(block_at(params, m, k, t) * BLK, BLK), BLK)
                scores[m, :, spot] = lax.dot_general(
                    left, cols[m, k, t], (((1,), (1,)), ((), ())), preferred_element_type=jnp.float32
                )


def finish_kernel(params, bins, scores, p0, p1, p2, p3, match, row_bins, col_bins, block, sems):
    alpha = bins[0]
    mine = params[3]
    lanes = lax.broadcasted_iota(jnp.int32, (1, 128), 1)
    row_id = lax.broadcasted_iota(jnp.int32, (BLK, 128), 0)
    quarter = lax.broadcasted_iota(jnp.int32, (4, 128), 0)
    side = jnp.zeros((4, 128), jnp.float32)
    edges = [jnp.zeros((4, 128), jnp.float32)] * NCH
    stores = []
    for m, pay in enumerate((p0, p1, p2, p3)):
        p = params[16 + m]
        n_rows = params[4 + m]
        n_cols = params[8 + m]
        both = n_rows.astype(jnp.float32) + n_cols.astype(jnp.float32)
        norm = -jnp.log(jnp.full((1, 128), both))
        line = pay[pl.ds(mine, 1), :]
        pot = jnp.transpose(jnp.broadcast_to(line, (BLK, 128)))
        row_kept = mine * BLK + row_id < n_rows
        line = jnp.where(mine * BLK + lanes < n_rows, alpha + line + pay[33:34, :] - norm, 0.0)
        side = jnp.where(quarter == p, line, side)
        for c in range(NCH):
            spot = pl.ds(c * 128, 128)
            col_pot = pay[NBLK + c : NBLK + c + 1, :]
            col_kept = c * 128 + lanes < n_cols
            tile = scores[m, :, spot] + pot + col_pot - norm
            block[m, :, spot] = jnp.where(row_kept & col_kept, tile, 0.0)
            line = jnp.where(col_kept, alpha + pay[32:33, :] + col_pot - norm, 0.0)
            edges[c] = jnp.where(quarter == p, line, edges[c])
        copy = pltpu.make_async_copy(block.at[m], match.at[p], sems.at[m])
        copy.start()
        stores.append(copy)
    row_bins[...] = side
    for c in range(NCH):
        col_bins[:, pl.ds(c * 128, 128)] = edges[c]
    for copy in stores:
        copy.wait()


SMEM = functools.partial(pl.BlockSpec, memory_space=pltpu.SMEM)
VMEM = functools.partial(pl.BlockSpec, memory_space=pltpu.VMEM)
ANY = functools.partial(pl.BlockSpec, memory_space=pl.ANY)


def run_sinkhorn(params, bins, xs):
    f32 = jnp.float32
    return pl.pallas_call(
        sinkhorn_kernel,
        out_shape=jax.ShapeDtypeStruct((40, 128), f32),
        in_specs=[SMEM()] * 2 + [ANY()] * 4,
        out_specs=VMEM(),
        scratch_shapes=[
            pltpu.VMEM((KP, KP), f32),
            pltpu.VMEM((BIG, KP), f32),
            pltpu.VMEM((BIG, KP), f32),
            pltpu.VMEM((KP, D), jnp.bfloat16),
            pltpu.VMEM((KP, D), jnp.bfloat16),
            pltpu.VMEM((2 * BIG, 128), f32),
            pltpu.VMEM((KP, 128), f32),
            pltpu.VMEM((KP, 128), f32),
            pltpu.VMEM((KP, 128), f32),
            pltpu.VMEM((KP, 128), f32),
            pltpu.VMEM((8, KP), f32),
            pltpu.VMEM((8, KP), f32),
            pltpu.SemaphoreType.DMA((4, 4, 2)),
        ],
        compiler_params=pltpu.CompilerParams(vmem_limit_bytes=40 * 1024 * 1024),
        cost_estimate=pl.CostEstimate(
            flops=200_000_000_000, bytes_accessed=2 << 20, transcendentals=0
        ),
        name="sinkhorn",
    )(params, bins, *xs)


def run_pick(index, counts, pairs, desc):
    part = jax.ShapeDtypeStruct((2, BLK, D), jnp.bfloat16)
    return pl.pallas_call(
        pick_kernel,
        out_shape=(part, part, part, part, jax.ShapeDtypeStruct((20,), jnp.int32)),
        in_specs=[SMEM()] * 3 + [ANY()],
        out_specs=[VMEM()] * 4 + [SMEM()],
        scratch_shapes=[pltpu.SemaphoreType.DMA((4, 2))],
        compiler_params=pltpu.CompilerParams(vmem_limit_bytes=4 * 1024 * 1024),
        name="pick",
    )(index, counts, pairs, desc)


def run_scores(params, desc, cs):
    return pl.pallas_call(
        score_kernel,
        out_shape=jax.ShapeDtypeStruct((4, BLK, KP), jnp.float32),
        in_specs=[SMEM(), VMEM()] + [ANY()] * 4,
        out_specs=VMEM(),
        scratch_shapes=[
            pltpu.VMEM((4, 4, 4, BLK, D), jnp.bfloat16),
            pltpu.SemaphoreType.DMA((4,)),
        ],
        compiler_params=pltpu.CompilerParams(vmem_limit_bytes=16 * 1024 * 1024),
        cost_estimate=pl.CostEstimate(
            flops=8_000_000_000, bytes_accessed=8 << 20, transcendentals=0
        ),
        name="scores",
    )(params, desc, *cs)


def run_finish(params, bins, scores, pays):
    f32 = jnp.float32
    return pl.pallas_call(
        finish_kernel,
        out_shape=(
            jax.ShapeDtypeStruct((4, BLK, KP), f32),
            jax.ShapeDtypeStruct((4, BLK), f32),
            jax.ShapeDtypeStruct((4, KP), f32),
        ),
        in_specs=[SMEM()] * 2 + [VMEM()] * 5,
        out_specs=(ANY(), VMEM(), VMEM()),
        scratch_shapes=[pltpu.VMEM((4, BLK, KP), f32), pltpu.SemaphoreType.DMA((4,))],
        compiler_params=pltpu.CompilerParams(vmem_limit_bytes=16 * 1024 * 1024),
        name="finish",
    )(params, bins, scores, *pays)


def shifts(groups, along_b):
    def perm(k):
        moves = []
        for g in range(groups):
            for i in range(4):
                for j in range(4):
                    on_row_1 = (g % 2 == 0) == along_b
                    to = (i, (j + k) % 4) if on_row_1 else ((i + k) % 4, j)
                    moves.append((g * 16 + i * 4 + j, g * 16 + to[0] * 4 + to[1]))
        return moves

    return perm


def on_device(descriptors, counts, pairs, bin_score):
    groups = lax.axis_size("pair")
    even = lax.axis_index("pair") % 2 == 0
    i, j = lax.axis_index("row_0"), lax.axis_index("row_1")
    a, b = jnp.where(even, i, j), jnp.where(even, j, i)
    by_b, by_a = shifts(groups, True), shifts(groups, False)

    index = jnp.stack([a, b, even.astype(jnp.int32), i * 4 + j]).astype(jnp.int32)
    s0, s1, s2, s3, params = run_pick(index, counts, pairs, descriptors)
    first = [s0] + [lax.ppermute(s, AXES, by_b(k)) for k, s in ((1, s1), (2, s2), (3, s3))]
    x0 = jnp.stack(first)
    xs = [x0] + [lax.ppermute(x0, AXES, by_a(k)) for k in (1, 2, 3)]
    c0 = jnp.stack([x[:, 1] for x in xs])
    cs = [c0] + [lax.ppermute(c0, AXES, by_b(k)) for k in (1, 2, 3)]
    pay = run_sinkhorn(params, bin_score, xs)
    pays = [pay] + [lax.ppermute(pay, AXES, by_b(k)) for k in (1, 2, 3)]
    desc, late = lax.optimization_barrier((descriptors, pay))
    scores = run_scores(params, desc, cs)
    return run_finish(params, bin_score, scores, [late] + pays[1:])


def solution(mesh):
    finer = Mesh(mesh.devices.reshape(mesh.shape["pair"], 4, 4), AXES)
    rows = ("row_0", "row_1")
    in_specs = (P("pair", rows, None), P("pair"), P("pair", None), P())
    out_specs = (P("pair", rows, None), P("pair", rows), P("pair", None))
    return jax.shard_map(
        on_device, mesh=finer, in_specs=in_specs, out_specs=out_specs, check_vma=False
    )
```

```python
import functools

import jax
import jax.numpy as jnp
from jax import lax
from jax.experimental import pallas as pl
from jax.experimental.pallas import tpu as pltpu
from jax.sharding import Mesh
from jax.sharding import PartitionSpec as P


ITERS = 10
KP = 2048
D = 256
BLK = 128
NBLK = KP // BLK
NCH = KP // 128
BIAS = 40.0
BIG = 256
SHARE = 8
AXES = ("pair", "row_0", "row_1")


def tree_sum(terms):
    while len(terms) > 1:
        pairs = [terms[k] + terms[k + 1] for k in range(0, len(terms) - 1, 2)]
        terms = pairs + ([terms[-1]] if len(terms) % 2 else [])
    return terms[0]


def sinkhorn_kernel(
    params, bins, x0, x1, x2, x3, out,
    kern, raw_0, raw_1, rows, cols, part, peak, wide_a, wide_mu, bin_hot, scale_b, share_b, sems,
):
    n_rows = params[4]
    n_cols = params[8]
    alpha = bins[0]
    copies = []
    for k, x in enumerate((x0, x1, x2, x3)):
        for t in range(4):
            spot = pl.ds(pl.multiple_of(block_at(params, k, t) * BLK, BLK), BLK)
            for side, target in ((1, cols), (0, rows)):
                copy = pltpu.make_async_copy(x.at[t, side], target.at[spot], sems.at[k, t, side])
                copy.start()
                copies.append(copy)
    lanes = lax.broadcasted_iota(jnp.int32, (1, 128), 1)
    row_count = jnp.full((8, 128), n_rows.astype(jnp.float32))
    col_count = jnp.full((8, 128), n_cols.astype(jnp.float32))
    mu = 1.0 / (row_count + col_count)
    mu_bin = col_count * mu
    nu_bin = row_count * mu
    for c in range(NCH):
        kept = jnp.broadcast_to(lanes + c * 128 < n_cols, (8, 128))
        scale_b[:, pl.ds(c * 128, 128)] = jnp.where(kept, 1.0, 0.0)
        share_b[:, pl.ds(c * 128, 128)] = jnp.where(kept, mu, 0.0)
    out[...] = jnp.zeros_like(out)
    pair_rows = 2 * BIG
    steps = (n_rows + pair_rows - 1) // pair_rows
    for copy in copies:
        copy.wait()

    @pl.loop(0, NBLK)
    def _(c):
        spot = pl.ds(pl.multiple_of(c * BLK, BLK), BLK)
        place = c * BLK + lax.broadcasted_iota(jnp.int32, (BLK, D), 0)
        kept = jnp.where(place < n_cols, 1.0, 0.0)
        cols[spot, :] = (cols[spot, :].astype(jnp.float32) * kept).astype(jnp.bfloat16)
        for g in range(0, BLK, 8):
            at = pl.ds(pl.multiple_of(c * BLK + g, 8), 8)
            row = c * BLK + g + lax.broadcasted_iota(jnp.int32, (8, 128), 0)
            wide_mu[at, :] = jnp.where(row < n_rows, mu, 0.0)

    def block(r):
        return pl.multiple_of(r * BIG, BIG)

    def scores_of(r, raw):
        left = rows[pl.ds(block(r), BIG), :] * jnp.bfloat16(0.0625)
        for c in range(NCH // 2):
            raw[:, pl.ds(c * 256, 256)] = lax.dot_general(
                left,
                cols[pl.ds(c * 256, 256), :],
                (((1,), (1,)), ((), ())),
                preferred_element_type=jnp.float32,
            )

    def exps_of(r, raw):
        base = block(r)
        for g in range(0, BIG, 8):
            at, near = pl.ds(base + g, 8), pl.ds(g, 8)
            tops = [raw[near, pl.ds(c * 128, 128)] for c in range(NCH)]
            while len(tops) > 1:
                tops = [jnp.maximum(tops[k], tops[k + 1]) for k in range(0, len(tops), 2)]
            drop = jnp.maximum(jnp.max(tops[0], axis=1, keepdims=True), alpha) - BIAS
            peak[at, :] = jnp.broadcast_to(drop, (8, 128))
        for g in range(0, BIG, 8):
            at, near = pl.ds(base + g, 8), pl.ds(g, 8)
            drop = peak[at, :]
            for c in range(NCH):
                ch = pl.ds(c * 128, 128)
                kern[at, ch] = jnp.exp(raw[near, ch] - drop)
            bin_hot[at, :] = jnp.where(lanes == 0, jnp.exp(alpha - drop), 0.0)

    scores_of(0, raw_0)

    @pl.loop(0, steps - 1)
    def _(m):
        scores_of(2 * m + 1, raw_1)
        exps_of(2 * m, raw_0)
        scores_of(2 * m + 2, raw_0)
        exps_of(2 * m + 1, raw_1)

    scores_of(2 * steps - 1, raw_1)
    exps_of(2 * steps - 2, raw_0)
    exps_of(2 * steps - 1, raw_1)

    def sums(r, bin_b, low):
        base = block(r)
        for q in range(0, BIG // 8, SHARE):
            sets = [pl.ds(base + 8 * (q + g), 8) for g in range(SHARE)]
            acc = [bin_hot[sets[g], :] * bin_b for g in range(SHARE)]
            for c in range(NCH):
                ch = pl.ds(c * 128, 128)
                b = scale_b[:, ch]
                for g in range(SHARE):
                    acc[g] = acc[g] + kern[sets[g], ch] * b
            for g in range(SHARE):
                part[pl.ds(low + 8 * (q + g), 8), :] = acc[g]

    def scales(r, low):
        base = block(r)
        for g in range(0, BIG, 8):
            at = pl.ds(base + g, 8)
            total = jnp.sum(part[pl.ds(low + g, 8), :], axis=1, keepdims=True)
            wide_a[at, :] = wide_mu[at, :] / jnp.broadcast_to(total, (8, 128))

    def gathers(r, acc):
        acc = list(acc)
        base = block(r)
        for g in range(0, BIG, 8):
            at = pl.ds(base + g, 8)
            a = wide_a[at, :]
            for c in range(NCH):
                acc[c] = acc[c] + kern[at, pl.ds(c * 128, 128)] * a
            acc[NCH] = acc[NCH] + bin_hot[at, :] * a
        return tuple(acc)

    def sweep(_, carry):
        bin_b, _ = carry
        whole = tree_sum([scale_b[:, pl.ds(c * 128, 128)] for c in range(NCH)])
        whole = jnp.broadcast_to(jnp.sum(whole, axis=1, keepdims=True), (8, 128))
        bin_line = mu_bin / (whole + bin_b)
        sums(0, bin_b, 0)

        @pl.loop(0, steps - 1)
        def _(m):
            sums(2 * m + 1, bin_b, BIG)
            scales(2 * m, 0)
            sums(2 * m + 2, bin_b, 0)
            scales(2 * m + 1, BIG)

        sums(2 * steps - 1, bin_b, BIG)
        scales(2 * steps - 2, 0)
        scales(2 * steps - 1, BIG)
        zero = jnp.zeros((8, 128), jnp.float32)
        acc = lax.fori_loop(0, 2 * steps, gathers, (zero,) * (NCH + 1))
        for c in range(NCH):
            ch = pl.ds(c * 128, 128)
            total = jnp.broadcast_to(jnp.sum(acc[c], axis=0, keepdims=True), (8, 128))
            scale_b[:, ch] = share_b[:, ch] / (total + bin_line)
        bin_acc = jnp.broadcast_to(jnp.sum(acc[NCH], axis=0, keepdims=True), (8, 128))
        bin_sum = jnp.broadcast_to(jnp.sum(bin_acc, axis=1, keepdims=True), (8, 128))
        return nu_bin / (bin_sum + bin_line), bin_line

    ones = jnp.ones((8, 128), jnp.float32)
    bin_b, bin_line = lax.fori_loop(0, ITERS, sweep, (ones, ones))

    @pl.loop(0, (n_rows + BLK - 1) // BLK)
    def _(r):
        spot = pl.ds(pl.multiple_of(r * BLK, BLK), BLK)
        pot = jnp.log(wide_a[spot, :]) - peak[spot, :]
        out[pl.ds(r, 1), :] = jnp.transpose(pot)[:1]

    for c in range(NCH):
        out[NBLK + c : NBLK + c + 1, :] = jnp.log(scale_b[0:1, pl.ds(c * 128, 128)])
    out[32:33, :] = (jnp.log(bin_line) - alpha)[:1]
    out[33:34, :] = jnp.log(bin_b)[:1]


def block_at(params, k, t):
    a = lax.rem(params[0] - k + 4, 4)
    b = lax.rem(params[1] - t + 4, 4)
    return jnp.where(params[2] == 1, a * 4 + b, b * 4 + a)


def pick_kernel(index, counts, pairs, desc, s0, s1, s2, s3, e0, e1, e2, e3, params, sems, more_sems):
    b = index[1]
    copies = []
    for k, target in ((1, s1), (2, s2), (3, s3), (0, s0)):
        p = lax.rem(b + k, 4)
        for side in range(2):
            copy = pltpu.make_async_copy(desc.at[pairs[p, side]], target.at[side], sems.at[k, side])
            copy.start()
            copies.append(copy)
    for k, target in ((1, e1), (2, e2), (3, e3), (0, e0)):
        for m in (1, 2, 3):
            p = lax.rem(b + k - m + 4, 4)
            copy = pltpu.make_async_copy(
                desc.at[pairs[p, 1]], target.at[m - 1], more_sems.at[k, m - 1]
            )
            copy.start()
            copies.append(copy)
    for c in range(4):
        params[c] = index[c]
    for m in range(4):
        p = lax.rem(b - m + 4, 4)
        params[4 + m] = counts[pairs[p, 0]]
        params[8 + m] = counts[pairs[p, 1]]
        params[12 + m] = pairs[p, 0]
        params[16 + m] = p
    for copy in copies:
        copy.wait()


def score_kernel(params, desc, x0, x1, x2, x3, y0, y1, y2, y3, scores, own, others, sems):
    loads = []
    for k, x in enumerate((x0, x1, x2, x3)):
        loads.append(pltpu.make_async_copy(x.at[:, 1], own.at[k], sems.at[0, k]))
    for k, y in enumerate((y0, y1, y2, y3)):
        loads.append(pltpu.make_async_copy(y, others.at[k], sems.at[1, k]))
    for copy in loads:
        copy.start()
    lefts = [desc[params[12 + m]] * jnp.bfloat16(0.0625) for m in range(4)]
    for k in range(4):
        loads[k].wait()
        loads[4 + k].wait()
        for t in range(4):
            spot = pl.ds(pl.multiple_of(block_at(params, k, t) * BLK, BLK), BLK)
            for m in range(4):
                scores[m, :, spot] = lax.dot_general(
                    lefts[m],
                    own[k, t] if m == 0 else others[k, t, m - 1],
                    (((1,), (1,)), ((), ())),
                    preferred_element_type=jnp.float32,
                )


def finish_kernel(params, bins, scores, p0, p1, p2, p3, match, row_bins, col_bins, block, sems):
    alpha = bins[0]
    mine = params[3]
    lanes = lax.broadcasted_iota(jnp.int32, (1, 128), 1)
    row_id = lax.broadcasted_iota(jnp.int32, (BLK, 128), 0)
    quarter = lax.broadcasted_iota(jnp.int32, (4, 128), 0)
    side = jnp.zeros((4, 128), jnp.float32)
    edges = [jnp.zeros((4, 128), jnp.float32)] * NCH
    stores = []
    for m, pay in enumerate((p0, p1, p2, p3)):
        p = params[16 + m]
        n_rows = params[4 + m]
        n_cols = params[8 + m]
        both = n_rows.astype(jnp.float32) + n_cols.astype(jnp.float32)
        norm = -jnp.log(jnp.full((1, 128), both))
        line = pay[pl.ds(mine, 1), :]
        pot = jnp.transpose(jnp.broadcast_to(line, (BLK, 128)))
        row_kept = mine * BLK + row_id < n_rows
        line = jnp.where(mine * BLK + lanes < n_rows, alpha + line + pay[33:34, :] - norm, 0.0)
        side = jnp.where(quarter == p, line, side)
        for c in range(NCH):
            spot = pl.ds(c * 128, 128)
            col_pot = pay[NBLK + c : NBLK + c + 1, :]
            col_kept = c * 128 + lanes < n_cols
            tile = scores[m, :, spot] + pot + col_pot - norm
            block[m, :, spot] = jnp.where(row_kept & col_kept, tile, 0.0)
            line = jnp.where(col_kept, alpha + pay[32:33, :] + col_pot - norm, 0.0)
            edges[c] = jnp.where(quarter == p, line, edges[c])
        copy = pltpu.make_async_copy(block.at[m], match.at[p], sems.at[m])
        copy.start()
        stores.append(copy)
    row_bins[...] = side
    for c in range(NCH):
        col_bins[:, pl.ds(c * 128, 128)] = edges[c]
    for copy in stores:
        copy.wait()


SMEM = functools.partial(pl.BlockSpec, memory_space=pltpu.SMEM)
VMEM = functools.partial(pl.BlockSpec, memory_space=pltpu.VMEM)
ANY = functools.partial(pl.BlockSpec, memory_space=pl.ANY)


def run_sinkhorn(params, bins, xs):
    f32 = jnp.float32
    return pl.pallas_call(
        sinkhorn_kernel,
        out_shape=jax.ShapeDtypeStruct((40, 128), f32),
        in_specs=[SMEM()] * 2 + [ANY()] * 4,
        out_specs=VMEM(),
        scratch_shapes=[
            pltpu.VMEM((KP, KP), f32),
            pltpu.VMEM((BIG, KP), f32),
            pltpu.VMEM((BIG, KP), f32),
            pltpu.VMEM((KP, D), jnp.bfloat16),
            pltpu.VMEM((KP, D), jnp.bfloat16),
            pltpu.VMEM((2 * BIG, 128), f32),
            pltpu.VMEM((KP, 128), f32),
            pltpu.VMEM((KP, 128), f32),
            pltpu.VMEM((KP, 128), f32),
            pltpu.VMEM((KP, 128), f32),
            pltpu.VMEM((8, KP), f32),
            pltpu.VMEM((8, KP), f32),
            pltpu.SemaphoreType.DMA((4, 4, 2)),
        ],
        compiler_params=pltpu.CompilerParams(vmem_limit_bytes=40 * 1024 * 1024),
        cost_estimate=pl.CostEstimate(
            flops=200_000_000_000, bytes_accessed=2 << 20, transcendentals=0
        ),
        name="sinkhorn",
    )(params, bins, *xs)


def run_pick(index, counts, pairs, desc):
    part = jax.ShapeDtypeStruct((2, BLK, D), jnp.bfloat16)
    more = jax.ShapeDtypeStruct((3, BLK, D), jnp.bfloat16)
    return pl.pallas_call(
        pick_kernel,
        out_shape=(part,) * 4 + (more,) * 4 + (jax.ShapeDtypeStruct((20,), jnp.int32),),
        in_specs=[SMEM()] * 3 + [ANY()],
        out_specs=[VMEM()] * 8 + [SMEM()],
        scratch_shapes=[pltpu.SemaphoreType.DMA((4, 2)), pltpu.SemaphoreType.DMA((4, 3))],
        compiler_params=pltpu.CompilerParams(vmem_limit_bytes=6 * 1024 * 1024),
        name="pick",
    )(index, counts, pairs, desc)


def run_scores(params, desc, xs, ys):
    return pl.pallas_call(
        score_kernel,
        out_shape=jax.ShapeDtypeStruct((4, BLK, KP), jnp.float32),
        in_specs=[SMEM(), VMEM()] + [ANY()] * 8,
        out_specs=VMEM(),
        scratch_shapes=[
            pltpu.VMEM((4, 4, BLK, D), jnp.bfloat16),
            pltpu.VMEM((4, 4, 3, BLK, D), jnp.bfloat16),
            pltpu.SemaphoreType.DMA((2, 4)),
        ],
        compiler_params=pltpu.CompilerParams(vmem_limit_bytes=16 * 1024 * 1024),
        cost_estimate=pl.CostEstimate(
            flops=8_000_000_000, bytes_accessed=8 << 20, transcendentals=0
        ),
        name="scores",
    )(params, desc, *xs, *ys)


def run_finish(params, bins, scores, pays):
    f32 = jnp.float32
    return pl.pallas_call(
        finish_kernel,
        out_shape=(
            jax.ShapeDtypeStruct((4, BLK, KP), f32),
            jax.ShapeDtypeStruct((4, BLK), f32),
            jax.ShapeDtypeStruct((4, KP), f32),
        ),
        in_specs=[SMEM()] * 2 + [VMEM()] * 5,
        out_specs=(ANY(), VMEM(), VMEM()),
        scratch_shapes=[pltpu.VMEM((4, BLK, KP), f32), pltpu.SemaphoreType.DMA((4,))],
        compiler_params=pltpu.CompilerParams(vmem_limit_bytes=16 * 1024 * 1024),
        name="finish",
    )(params, bins, scores, *pays)


def shifts(groups, along_b):
    def perm(k):
        moves = []
        for g in range(groups):
            for i in range(4):
                for j in range(4):
                    on_row_1 = (g % 2 == 0) == along_b
                    to = (i, (j + k) % 4) if on_row_1 else ((i + k) % 4, j)
                    moves.append((g * 16 + i * 4 + j, g * 16 + to[0] * 4 + to[1]))
        return moves

    return perm


def on_device(descriptors, counts, pairs, bin_score):
    groups = lax.axis_size("pair")
    even = lax.axis_index("pair") % 2 == 0
    i, j = lax.axis_index("row_0"), lax.axis_index("row_1")
    a, b = jnp.where(even, i, j), jnp.where(even, j, i)
    by_b, by_a = shifts(groups, True), shifts(groups, False)

    index = jnp.stack([a, b, even.astype(jnp.int32), i * 4 + j]).astype(jnp.int32)
    s0, s1, s2, s3, e0, e1, e2, e3, params = run_pick(index, counts, pairs, descriptors)

    def send(parts, moves):
        arrived = []
        for k, x in enumerate(parts, 1):
            arrived.append(lax.ppermute(x, AXES, moves(k)))
        return arrived

    x0 = jnp.stack([s0] + send((s1, s2, s3), by_b))
    xs = [x0] + send((x0, x0, x0), by_a)
    y0 = jnp.stack([e0] + send((e1, e2, e3), by_b))
    ys = [y0] + send((y0, y0, y0), by_a)
    pay = run_sinkhorn(params, bin_score, xs)
    pays = [pay] + [lax.ppermute(pay, AXES, by_b(k)) for k in (1, 2, 3)]
    desc, late = lax.optimization_barrier((descriptors, pay))
    scores = run_scores(params, desc, xs, ys)
    return run_finish(params, bin_score, scores, [late] + pays[1:])


def solution(mesh):
    finer = Mesh(mesh.devices.reshape(mesh.shape["pair"], 4, 4), AXES)
    rows = ("row_0", "row_1")
    in_specs = (P("pair", rows, None), P("pair"), P("pair", None), P())
    out_specs = (P("pair", rows, None), P("pair", rows), P("pair", None))
    return jax.shard_map(
        on_device, mesh=finer, in_specs=in_specs, out_specs=out_specs, check_vma=False
    )
```

```python
import functools

import jax
import jax.numpy as jnp
from jax import lax
from jax.experimental import pallas as pl
from jax.experimental.pallas import tpu as pltpu
from jax.sharding import Mesh
from jax.sharding import PartitionSpec as P


ITERS = 10
KP = 2048
D = 256
BLK = 128
NBLK = KP // BLK
NCH = KP // 128
BIAS = 40.0
BIG = 256
SHARE = 8
AXES = ("pair", "row_0", "row_1")


def tree_sum(terms):
    while len(terms) > 1:
        pairs = [terms[k] + terms[k + 1] for k in range(0, len(terms) - 1, 2)]
        terms = pairs + ([terms[-1]] if len(terms) % 2 else [])
    return terms[0]


def sinkhorn_kernel(
    params, bins, x0, x1, x2, x3, out,
    kern, raw_0, raw_1, rows, cols, part, peak, wide_a, wide_mu, bin_hot, scale_b, share_b, sems,
):
    n_rows = params[4]
    n_cols = params[8]
    alpha = bins[0]
    copies = []
    for k, x in enumerate((x0, x1, x2, x3)):
        for t in range(4):
            spot = pl.ds(pl.multiple_of(block_at(params, k, t) * BLK, BLK), BLK)
            for side, target in ((1, cols), (0, rows)):
                copy = pltpu.make_async_copy(x.at[t, side], target.at[spot], sems.at[k, t, side])
                copy.start()
                copies.append(copy)
    lanes = lax.broadcasted_iota(jnp.int32, (1, 128), 1)
    row_count = jnp.full((8, 128), n_rows.astype(jnp.float32))
    col_count = jnp.full((8, 128), n_cols.astype(jnp.float32))
    mu = 1.0 / (row_count + col_count)
    mu_bin = col_count * mu
    nu_bin = row_count * mu
    for c in range(NCH):
        kept = jnp.broadcast_to(lanes + c * 128 < n_cols, (8, 128))
        scale_b[:, pl.ds(c * 128, 128)] = jnp.where(kept, 1.0, 0.0)
        share_b[:, pl.ds(c * 128, 128)] = jnp.where(kept, mu, 0.0)
    out[...] = jnp.zeros_like(out)
    pair_rows = 2 * BIG
    steps = (n_rows + pair_rows - 1) // pair_rows

    @pl.loop(0, NBLK)
    def _(c):
        for g in range(0, BLK, 8):
            at = pl.ds(pl.multiple_of(c * BLK + g, 8), 8)
            row = c * BLK + g + lax.broadcasted_iota(jnp.int32, (8, 128), 0)
            wide_mu[at, :] = jnp.where(row < n_rows, mu, 0.0)

    for copy in copies:
        copy.wait()

    @pl.loop(n_cols // BLK, NBLK)
    def _(c):
        spot = pl.ds(pl.multiple_of(c * BLK, BLK), BLK)
        place = c * BLK + lax.broadcasted_iota(jnp.int32, (BLK, D), 0)
        kept = jnp.where(place < n_cols, 1.0, 0.0)
        cols[spot, :] = (cols[spot, :].astype(jnp.float32) * kept).astype(jnp.bfloat16)

    def block(r):
        return pl.multiple_of(r * BIG, BIG)

    def scores_of(r, raw):
        left = rows[pl.ds(block(r), BIG), :] * jnp.bfloat16(0.0625)
        for c in range(NCH // 2):
            raw[:, pl.ds(c * 256, 256)] = lax.dot_general(
                left,
                cols[pl.ds(c * 256, 256), :],
                (((1,), (1,)), ((), ())),
                preferred_element_type=jnp.float32,
            )

    def exps_of(r, raw):
        base = block(r)
        for g in range(0, BIG, 8):
            at, near = pl.ds(base + g, 8), pl.ds(g, 8)
            tops = [raw[near, pl.ds(c * 128, 128)] for c in range(NCH)]
            while len(tops) > 1:
                tops = [jnp.maximum(tops[k], tops[k + 1]) for k in range(0, len(tops), 2)]
            drop = jnp.maximum(jnp.max(tops[0], axis=1, keepdims=True), alpha) - BIAS
            peak[at, :] = jnp.broadcast_to(drop, (8, 128))
        for g in range(0, BIG, 8):
            at, near = pl.ds(base + g, 8), pl.ds(g, 8)
            drop = peak[at, :]
            for c in range(NCH):
                ch = pl.ds(c * 128, 128)
                kern[at, ch] = jnp.exp(raw[near, ch] - drop)
            bin_hot[at, :] = jnp.where(lanes == 0, jnp.exp(alpha - drop), 0.0)

    scores_of(0, raw_0)
    once = jnp.minimum(n_cols, 1)

    @pl.loop(0, steps - 1)
    def _(m):
        @pl.loop(0, once)
        def _(_):
            scores_of(2 * m + 1, raw_1)
            exps_of(2 * m, raw_0)

        @pl.loop(0, once)
        def _(_):
            scores_of(2 * m + 2, raw_0)
            exps_of(2 * m + 1, raw_1)

    @pl.loop(0, once)
    def _(_):
        scores_of(2 * steps - 1, raw_1)
        exps_of(2 * steps - 2, raw_0)

    exps_of(2 * steps - 1, raw_1)

    def sums(r, bin_b, low):
        base = block(r)
        for q in range(0, BIG // 8, SHARE):
            sets = [pl.ds(base + 8 * (q + g), 8) for g in range(SHARE)]
            acc = [bin_hot[sets[g], :] * bin_b for g in range(SHARE)]
            for c in range(NCH):
                ch = pl.ds(c * 128, 128)
                b = scale_b[:, ch]
                for g in range(SHARE):
                    acc[g] = acc[g] + kern[sets[g], ch] * b
            for g in range(SHARE):
                part[pl.ds(low + 8 * (q + g), 8), :] = acc[g]

    def scales(r, low):
        base = block(r)
        for g in range(0, BIG, 8):
            at = pl.ds(base + g, 8)
            total = jnp.sum(part[pl.ds(low + g, 8), :], axis=1, keepdims=True)
            wide_a[at, :] = wide_mu[at, :] / jnp.broadcast_to(total, (8, 128))

    def gathers(r, acc):
        acc = list(acc)
        base = block(r)
        for g in range(0, BIG, 8):
            at = pl.ds(base + g, 8)
            a = wide_a[at, :]
            for c in range(NCH):
                acc[c] = acc[c] + kern[at, pl.ds(c * 128, 128)] * a
            acc[NCH] = acc[NCH] + bin_hot[at, :] * a
        return tuple(acc)

    def sweep(_, carry):
        bin_b, _ = carry
        whole = tree_sum([scale_b[:, pl.ds(c * 128, 128)] for c in range(NCH)])
        whole = jnp.broadcast_to(jnp.sum(whole, axis=1, keepdims=True), (8, 128))
        bin_line = mu_bin / (whole + bin_b)
        sums(0, bin_b, 0)

        @pl.loop(0, steps - 1)
        def _(m):
            sums(2 * m + 1, bin_b, BIG)
            scales(2 * m, 0)
            sums(2 * m + 2, bin_b, 0)
            scales(2 * m + 1, BIG)

        sums(2 * steps - 1, bin_b, BIG)
        scales(2 * steps - 2, 0)
        scales(2 * steps - 1, BIG)
        zero = jnp.zeros((8, 128), jnp.float32)
        acc = lax.fori_loop(0, 2 * steps, gathers, (zero,) * (NCH + 1))
        for c in range(NCH):
            ch = pl.ds(c * 128, 128)
            total = jnp.broadcast_to(jnp.sum(acc[c], axis=0, keepdims=True), (8, 128))
            scale_b[:, ch] = share_b[:, ch] / (total + bin_line)
        bin_acc = jnp.broadcast_to(jnp.sum(acc[NCH], axis=0, keepdims=True), (8, 128))
        bin_sum = jnp.broadcast_to(jnp.sum(bin_acc, axis=1, keepdims=True), (8, 128))
        return nu_bin / (bin_sum + bin_line), bin_line

    ones = jnp.ones((8, 128), jnp.float32)
    bin_b, bin_line = lax.fori_loop(0, ITERS, sweep, (ones, ones))

    @pl.loop(0, (n_rows + BLK - 1) // BLK)
    def _(r):
        spot = pl.ds(pl.multiple_of(r * BLK, BLK), BLK)
        pot = jnp.log(wide_a[spot, :]) - peak[spot, :]
        out[pl.ds(r, 1), :] = jnp.transpose(pot)[:1]

    for c in range(NCH):
        out[NBLK + c : NBLK + c + 1, :] = jnp.log(scale_b[0:1, pl.ds(c * 128, 128)])
    out[32:33, :] = (jnp.log(bin_line) - alpha)[:1]
    out[33:34, :] = jnp.log(bin_b)[:1]


def block_at(params, k, t):
    a = lax.rem(params[0] - k + 4, 4)
    b = lax.rem(params[1] - t + 4, 4)
    return jnp.where(params[2] == 1, a * 4 + b, b * 4 + a)


def pick_kernel(index, desc, s0, s1, s2, s3, e0, e1, e2, e3, params, sems, more_sems):
    b = index[1]

    def image(p, side):
        return index[12 + 2 * p + side]

    copies = []
    for k, target in ((1, s1), (2, s2), (3, s3), (0, s0)):
        p = lax.rem(b + k, 4)
        for side in range(2):
            copy = pltpu.make_async_copy(desc.at[image(p, side)], target.at[side], sems.at[k, side])
            copy.start()
            copies.append(copy)
    for k, target in ((1, e1), (2, e2), (3, e3), (0, e0)):
        for m in (1, 2, 3):
            p = lax.rem(b + k - m + 4, 4)
            copy = pltpu.make_async_copy(
                desc.at[image(p, 1)], target.at[m - 1], more_sems.at[k, m - 1]
            )
            copy.start()
            copies.append(copy)
    for c in range(4):
        params[c] = index[c]
    for m in range(4):
        p = lax.rem(b - m + 4, 4)
        params[4 + m] = index[4 + image(p, 0)]
        params[8 + m] = index[4 + image(p, 1)]
        params[12 + m] = image(p, 0)
        params[16 + m] = p
    for copy in copies:
        copy.wait()


def score_kernel(params, desc, x0, x1, x2, x3, y0, y1, y2, y3, scores, own, others, sems):
    loads = []
    for k, x in enumerate((x0, x1, x2, x3)):
        loads.append(pltpu.make_async_copy(x.at[:, 1], own.at[k], sems.at[0, k]))
    for k, y in enumerate((y0, y1, y2, y3)):
        loads.append(pltpu.make_async_copy(y, others.at[k], sems.at[1, k]))
    for copy in loads:
        copy.start()
    lefts = [desc[params[12 + m]] * jnp.bfloat16(0.0625) for m in range(4)]
    for k in range(4):
        loads[k].wait()
        loads[4 + k].wait()
        for t in range(4):
            spot = pl.ds(pl.multiple_of(block_at(params, k, t) * BLK, BLK), BLK)
            for m in range(4):
                scores[m, :, spot] = lax.dot_general(
                    lefts[m],
                    own[k, t] if m == 0 else others[k, t, m - 1],
                    (((1,), (1,)), ((), ())),
                    preferred_element_type=jnp.float32,
                )


def finish_kernel(params, bins, scores, p0, p1, p2, p3, match, row_bins, col_bins, block, sems):
    alpha = bins[0]
    mine = params[3]
    lanes = lax.broadcasted_iota(jnp.int32, (1, 128), 1)
    row_id = lax.broadcasted_iota(jnp.int32, (BLK, 128), 0)
    quarter = lax.broadcasted_iota(jnp.int32, (4, 128), 0)
    side = jnp.zeros((4, 128), jnp.float32)
    edges = [jnp.zeros((4, 128), jnp.float32)] * NCH
    stores = []
    for m, pay in enumerate((p0, p1, p2, p3)):
        p = params[16 + m]
        n_rows = params[4 + m]
        n_cols = params[8 + m]
        both = n_rows.astype(jnp.float32) + n_cols.astype(jnp.float32)
        norm = -jnp.log(jnp.full((1, 128), both))
        line = pay[pl.ds(mine, 1), :]
        pot = jnp.transpose(jnp.broadcast_to(line, (BLK, 128)))
        row_kept = mine * BLK + row_id < n_rows
        line = jnp.where(mine * BLK + lanes < n_rows, alpha + line + pay[33:34, :] - norm, 0.0)
        side = jnp.where(quarter == p, line, side)
        for c in range(NCH):
            spot = pl.ds(c * 128, 128)
            col_pot = pay[NBLK + c : NBLK + c + 1, :]
            col_kept = c * 128 + lanes < n_cols
            tile = scores[m, :, spot] + pot + col_pot - norm
            block[m, :, spot] = jnp.where(row_kept & col_kept, tile, 0.0)
            line = jnp.where(col_kept, alpha + pay[32:33, :] + col_pot - norm, 0.0)
            edges[c] = jnp.where(quarter == p, line, edges[c])
        copy = pltpu.make_async_copy(block.at[m], match.at[p], sems.at[m])
        copy.start()
        stores.append(copy)
    row_bins[...] = side
    for c in range(NCH):
        col_bins[:, pl.ds(c * 128, 128)] = edges[c]
    for copy in stores:
        copy.wait()


SMEM = functools.partial(pl.BlockSpec, memory_space=pltpu.SMEM)
VMEM = functools.partial(pl.BlockSpec, memory_space=pltpu.VMEM)
ANY = functools.partial(pl.BlockSpec, memory_space=pl.ANY)


def run_sinkhorn(params, bins, xs):
    f32 = jnp.float32
    return pl.pallas_call(
        sinkhorn_kernel,
        out_shape=jax.ShapeDtypeStruct((40, 128), f32),
        in_specs=[SMEM()] * 2 + [ANY()] * 4,
        out_specs=VMEM(),
        scratch_shapes=[
            pltpu.VMEM((KP, KP), f32),
            pltpu.VMEM((BIG, KP), f32),
            pltpu.VMEM((BIG, KP), f32),
            pltpu.VMEM((KP, D), jnp.bfloat16),
            pltpu.VMEM((KP, D), jnp.bfloat16),
            pltpu.VMEM((2 * BIG, 128), f32),
            pltpu.VMEM((KP, 128), f32),
            pltpu.VMEM((KP, 128), f32),
            pltpu.VMEM((KP, 128), f32),
            pltpu.VMEM((KP, 128), f32),
            pltpu.VMEM((8, KP), f32),
            pltpu.VMEM((8, KP), f32),
            pltpu.SemaphoreType.DMA((4, 4, 2)),
        ],
        compiler_params=pltpu.CompilerParams(vmem_limit_bytes=40 * 1024 * 1024),
        cost_estimate=pl.CostEstimate(
            flops=200_000_000_000, bytes_accessed=2 << 20, transcendentals=0
        ),
        name="sinkhorn",
    )(params, bins, *xs)


def run_pick(index, desc):
    part = jax.ShapeDtypeStruct((2, BLK, D), jnp.bfloat16)
    more = jax.ShapeDtypeStruct((3, BLK, D), jnp.bfloat16)
    return pl.pallas_call(
        pick_kernel,
        out_shape=(part,) * 4 + (more,) * 4 + (jax.ShapeDtypeStruct((20,), jnp.int32),),
        in_specs=[SMEM(), ANY()],
        out_specs=[VMEM()] * 8 + [SMEM()],
        scratch_shapes=[pltpu.SemaphoreType.DMA((4, 2)), pltpu.SemaphoreType.DMA((4, 3))],
        compiler_params=pltpu.CompilerParams(vmem_limit_bytes=6 * 1024 * 1024),
        name="pick",
    )(index, desc)


def run_scores(params, desc, xs, ys):
    return pl.pallas_call(
        score_kernel,
        out_shape=jax.ShapeDtypeStruct((4, BLK, KP), jnp.float32),
        in_specs=[SMEM(), VMEM()] + [ANY()] * 8,
        out_specs=VMEM(),
        scratch_shapes=[
            pltpu.VMEM((4, 4, BLK, D), jnp.bfloat16),
            pltpu.VMEM((4, 4, 3, BLK, D), jnp.bfloat16),
            pltpu.SemaphoreType.DMA((2, 4)),
        ],
        compiler_params=pltpu.CompilerParams(vmem_limit_bytes=16 * 1024 * 1024),
        cost_estimate=pl.CostEstimate(
            flops=8_000_000_000, bytes_accessed=8 << 20, transcendentals=0
        ),
        name="scores",
    )(params, desc, *xs, *ys)


def run_finish(params, bins, scores, pays):
    f32 = jnp.float32
    return pl.pallas_call(
        finish_kernel,
        out_shape=(
            jax.ShapeDtypeStruct((4, BLK, KP), f32),
            jax.ShapeDtypeStruct((4, BLK), f32),
            jax.ShapeDtypeStruct((4, KP), f32),
        ),
        in_specs=[SMEM()] * 2 + [VMEM()] * 5,
        out_specs=(ANY(), VMEM(), VMEM()),
        scratch_shapes=[pltpu.VMEM((4, BLK, KP), f32), pltpu.SemaphoreType.DMA((4,))],
        compiler_params=pltpu.CompilerParams(vmem_limit_bytes=16 * 1024 * 1024),
        name="finish",
    )(params, bins, scores, *pays)


def shifts(groups, along_b):
    def perm(k):
        moves = []
        for g in range(groups):
            for i in range(4):
                for j in range(4):
                    on_row_1 = (g % 2 == 0) == along_b
                    to = (i, (j + k) % 4) if on_row_1 else ((i + k) % 4, j)
                    moves.append((g * 16 + i * 4 + j, g * 16 + to[0] * 4 + to[1]))
        return moves

    return perm


def on_device(descriptors, counts, pairs, bin_score):
    groups = lax.axis_size("pair")
    even = lax.axis_index("pair") % 2 == 0
    i, j = lax.axis_index("row_0"), lax.axis_index("row_1")
    a, b = jnp.where(even, i, j), jnp.where(even, j, i)
    by_b, by_a = shifts(groups, True), shifts(groups, False)

    index = jnp.stack([a, b, even.astype(jnp.int32), i * 4 + j]).astype(jnp.int32)
    index = jnp.concatenate([index, counts, pairs.reshape(-1)])
    s0, s1, s2, s3, e0, e1, e2, e3, params = run_pick(index, descriptors)

    def send(parts, moves):
        arrived = []
        for k, x in enumerate(parts, 1):
            arrived.append(lax.ppermute(x, AXES, moves(k)))
        return arrived

    x0 = jnp.stack([s0] + send((s1, s2, s3), by_b))
    xs = [x0] + send((x0, x0, x0), by_a)
    y0 = jnp.stack([e0] + send((e1, e2, e3), by_b))
    ys = [y0] + send((y0, y0, y0), by_a)
    pay = run_sinkhorn(params, bin_score, xs)
    pays = [pay] + [lax.ppermute(pay, AXES, by_b(k)) for k in (1, 2, 3)]
    desc, late = lax.optimization_barrier((descriptors, pay))
    scores = run_scores(params, desc, xs, ys)
    return run_finish(params, bin_score, scores, [late] + pays[1:])


def solution(mesh):
    finer = Mesh(mesh.devices.reshape(mesh.shape["pair"], 4, 4), AXES)
    rows = ("row_0", "row_1")
    in_specs = (P("pair", rows, None), P("pair"), P("pair", None), P())
    out_specs = (P("pair", rows, None), P("pair", rows), P("pair", None))
    return jax.shard_map(
        on_device, mesh=finer, in_specs=in_specs, out_specs=out_specs, check_vma=False
    )
```

```python
import functools

import jax
import jax.numpy as jnp
from jax import lax
from jax.experimental import pallas as pl
from jax.experimental.pallas import tpu as pltpu
from jax.sharding import Mesh
from jax.sharding import PartitionSpec as P


ITERS = 10
KP = 2048
D = 256
BLK = 128
NBLK = KP // BLK
NCH = KP // 128
BIAS = 40.0
BIG = 256
SHARE = 8
AXES = ("pair", "row_0", "row_1")


def tree_sum(terms):
    while len(terms) > 1:
        pairs = [terms[k] + terms[k + 1] for k in range(0, len(terms) - 1, 2)]
        terms = pairs + ([terms[-1]] if len(terms) % 2 else [])
    return terms[0]


def sinkhorn_kernel(
    params, bins, x0, x1, x2, x3, out,
    kern, raw_0, raw_1, rows, cols, part, peak, wide_a, wide_mu, bin_hot, scale_b, share_b, sems,
):
    n_rows = params[4]
    n_cols = params[8]
    alpha = bins[0]
    copies = []
    for k, x in enumerate((x0, x1, x2, x3)):
        for t in range(4):
            spot = pl.ds(pl.multiple_of(block_at(params, k, t) * BLK, BLK), BLK)
            for side, target in ((1, cols), (0, rows)):
                copy = pltpu.make_async_copy(x.at[t, side], target.at[spot], sems.at[k, t, side])
                copy.start()
                copies.append(copy)
    lanes = lax.broadcasted_iota(jnp.int32, (1, 128), 1)
    row_count = jnp.full((8, 128), n_rows.astype(jnp.float32))
    col_count = jnp.full((8, 128), n_cols.astype(jnp.float32))
    mu = 1.0 / (row_count + col_count)
    mu_bin = col_count * mu
    nu_bin = row_count * mu
    for c in range(NCH):
        kept = jnp.broadcast_to(lanes + c * 128 < n_cols, (8, 128))
        scale_b[:, pl.ds(c * 128, 128)] = jnp.where(kept, 1.0, 0.0)
        share_b[:, pl.ds(c * 128, 128)] = jnp.where(kept, mu, 0.0)
    out[...] = jnp.zeros_like(out)
    pair_rows = 2 * BIG
    steps = (n_rows + pair_rows - 1) // pair_rows

    @pl.loop(0, NBLK)
    def _(c):
        for g in range(0, BLK, 8):
            at = pl.ds(pl.multiple_of(c * BLK + g, 8), 8)
            row = c * BLK + g + lax.broadcasted_iota(jnp.int32, (8, 128), 0)
            wide_mu[at, :] = jnp.where(row < n_rows, mu, 0.0)

    for copy in copies:
        copy.wait()

    @pl.loop(n_cols // BLK, NBLK)
    def _(c):
        spot = pl.ds(pl.multiple_of(c * BLK, BLK), BLK)
        place = c * BLK + lax.broadcasted_iota(jnp.int32, (BLK, D), 0)
        kept = jnp.where(place < n_cols, 1.0, 0.0)
        cols[spot, :] = (cols[spot, :].astype(jnp.float32) * kept).astype(jnp.bfloat16)

    def block(r):
        return pl.multiple_of(r * BIG, BIG)

    def scores_of(r, raw):
        left = rows[pl.ds(block(r), BIG), :] * jnp.bfloat16(0.0625)
        for c in range(NCH // 2):
            raw[:, pl.ds(c * 256, 256)] = lax.dot_general(
                left,
                cols[pl.ds(c * 256, 256), :],
                (((1,), (1,)), ((), ())),
                preferred_element_type=jnp.float32,
            )

    def exps_of(r, raw):
        base = block(r)
        for g in range(0, BIG, 8):
            at, near = pl.ds(base + g, 8), pl.ds(g, 8)
            tops = [raw[near, pl.ds(c * 128, 128)] for c in range(NCH)]
            while len(tops) > 1:
                tops = [jnp.maximum(tops[k], tops[k + 1]) for k in range(0, len(tops), 2)]
            drop = jnp.maximum(jnp.max(tops[0], axis=1, keepdims=True), alpha) - BIAS
            peak[at, :] = jnp.broadcast_to(drop, (8, 128))
        for g in range(0, BIG, 8):
            at, near = pl.ds(base + g, 8), pl.ds(g, 8)
            drop = peak[at, :]
            for c in range(NCH):
                ch = pl.ds(c * 128, 128)
                kern[at, ch] = jnp.exp(raw[near, ch] - drop)
            bin_hot[at, :] = jnp.where(lanes == 0, jnp.exp(alpha - drop), 0.0)

    scores_of(0, raw_0)
    once = jnp.minimum(n_cols, 1)

    @pl.loop(0, steps - 1)
    def _(m):
        @pl.loop(0, once)
        def _(_):
            scores_of(2 * m + 1, raw_1)
            exps_of(2 * m, raw_0)

        @pl.loop(0, once)
        def _(_):
            scores_of(2 * m + 2, raw_0)
            exps_of(2 * m + 1, raw_1)

    @pl.loop(0, once)
    def _(_):
        scores_of(2 * steps - 1, raw_1)
        exps_of(2 * steps - 2, raw_0)

    exps_of(2 * steps - 1, raw_1)

    def sums(r, bin_b, low):
        base = block(r)
        for q in range(0, BIG // 8, SHARE):
            sets = [pl.ds(base + 8 * (q + g), 8) for g in range(SHARE)]
            acc = [bin_hot[sets[g], :] * bin_b for g in range(SHARE)]
            for c in range(NCH):
                ch = pl.ds(c * 128, 128)
                b = scale_b[:, ch]
                for g in range(SHARE):
                    acc[g] = acc[g] + kern[sets[g], ch] * b
            for g in range(SHARE):
                part[pl.ds(low + 8 * (q + g), 8), :] = acc[g]

    def scales(r, low):
        base = block(r)
        for g in range(0, BIG, 8):
            at = pl.ds(base + g, 8)
            total = jnp.sum(part[pl.ds(low + g, 8), :], axis=1, keepdims=True)
            wide_a[at, :] = wide_mu[at, :] / jnp.broadcast_to(total, (8, 128))

    def gathers(r, acc):
        acc = list(acc)
        base = block(r)
        for g in range(0, BIG, 8):
            at = pl.ds(base + g, 8)
            a = wide_a[at, :]
            for c in range(NCH):
                acc[c] = acc[c] + kern[at, pl.ds(c * 128, 128)] * a
            acc[NCH] = acc[NCH] + bin_hot[at, :] * a
        return tuple(acc)

    def sweep(_, carry):
        bin_b, _ = carry
        whole = tree_sum([scale_b[:, pl.ds(c * 128, 128)] for c in range(NCH)])
        whole = jnp.broadcast_to(jnp.sum(whole, axis=1, keepdims=True), (8, 128))
        bin_line = mu_bin / (whole + bin_b)
        sums(0, bin_b, 0)

        @pl.loop(0, steps - 1)
        def _(m):
            sums(2 * m + 1, bin_b, BIG)
            scales(2 * m, 0)
            sums(2 * m + 2, bin_b, 0)
            scales(2 * m + 1, BIG)

        sums(2 * steps - 1, bin_b, BIG)
        scales(2 * steps - 2, 0)
        scales(2 * steps - 1, BIG)
        zero = jnp.zeros((8, 128), jnp.float32)
        acc = lax.fori_loop(0, 2 * steps, gathers, (zero,) * (NCH + 1))
        for c in range(NCH):
            ch = pl.ds(c * 128, 128)
            total = jnp.broadcast_to(jnp.sum(acc[c], axis=0, keepdims=True), (8, 128))
            scale_b[:, ch] = share_b[:, ch] / (total + bin_line)
        bin_acc = jnp.broadcast_to(jnp.sum(acc[NCH], axis=0, keepdims=True), (8, 128))
        bin_sum = jnp.broadcast_to(jnp.sum(bin_acc, axis=1, keepdims=True), (8, 128))
        return nu_bin / (bin_sum + bin_line), bin_line

    ones = jnp.ones((8, 128), jnp.float32)
    bin_b, bin_line = lax.fori_loop(0, ITERS, sweep, (ones, ones))

    @pl.loop(0, (n_rows + BLK - 1) // BLK)
    def _(r):
        spot = pl.ds(pl.multiple_of(r * BLK, BLK), BLK)
        pot = jnp.log(wide_a[spot, :]) - peak[spot, :]
        out[pl.ds(r, 1), :] = jnp.transpose(pot)[:1]

    for c in range(NCH):
        out[NBLK + c : NBLK + c + 1, :] = jnp.log(scale_b[0:1, pl.ds(c * 128, 128)])
    out[32:33, :] = (jnp.log(bin_line) - alpha)[:1]
    out[33:34, :] = jnp.log(bin_b)[:1]


def block_at(params, k, t):
    a = lax.rem(params[0] - k + 4, 4)
    b = lax.rem(params[1] - t + 4, 4)
    return jnp.where(params[2] == 1, a * 4 + b, b * 4 + a)


def pick_kernel(index, desc, s0, s1, s2, s3, e0, e1, e2, e3, params, sems, more_sems):
    b = index[1]

    def image(p, side):
        return index[12 + 2 * p + side]

    copies = []
    for k, target in ((1, s1), (2, s2), (3, s3), (0, s0)):
        p = lax.rem(b + k, 4)
        for side in range(2):
            copy = pltpu.make_async_copy(desc.at[image(p, side)], target.at[side], sems.at[k, side])
            copy.start()
            copies.append(copy)
    for k, target in ((1, e1), (2, e2), (3, e3), (0, e0)):
        for m in (1, 2, 3):
            p = lax.rem(b + k - m + 4, 4)
            copy = pltpu.make_async_copy(
                desc.at[image(p, 1)], target.at[m - 1], more_sems.at[k, m - 1]
            )
            copy.start()
            copies.append(copy)
    for c in range(4):
        params[c] = index[c]
    for m in range(4):
        p = lax.rem(b - m + 4, 4)
        params[4 + m] = index[4 + image(p, 0)]
        params[8 + m] = index[4 + image(p, 1)]
        params[12 + m] = image(p, 0)
        params[16 + m] = p
    for copy in copies:
        copy.wait()


def score_kernel(params, desc, x0, x1, x2, x3, y0, y1, y2, y3, scores, own, others, sems):
    loads = []
    for k, x in enumerate((x0, x1, x2, x3)):
        loads.append(pltpu.make_async_copy(x.at[:, 1], own.at[k], sems.at[0, k]))
    for k, y in enumerate((y0, y1, y2, y3)):
        loads.append(pltpu.make_async_copy(y, others.at[k], sems.at[1, k]))
    for copy in loads:
        copy.start()
    lefts = [desc[params[12 + m]] * jnp.bfloat16(0.0625) for m in range(4)]
    for k in range(4):
        loads[k].wait()
        loads[4 + k].wait()
        for t in range(4):
            spot = pl.ds(pl.multiple_of(block_at(params, k, t) * BLK, BLK), BLK)
            for m in range(4):
                scores[m, :, spot] = lax.dot_general(
                    lefts[m],
                    own[k, t] if m == 0 else others[k, t, m - 1],
                    (((1,), (1,)), ((), ())),
                    preferred_element_type=jnp.float32,
                )


def finish_kernel(params, bins, scores, p0, p1, p2, p3, match, row_bins, col_bins, block, sems):
    alpha = bins[0]
    mine = params[3]
    lanes = lax.broadcasted_iota(jnp.int32, (1, 128), 1)
    row_id = lax.broadcasted_iota(jnp.int32, (BLK, 128), 0)
    quarter = lax.broadcasted_iota(jnp.int32, (4, 128), 0)
    side = jnp.zeros((4, 128), jnp.float32)
    edges = [jnp.zeros((4, 128), jnp.float32)] * NCH
    stores = []
    for m, pay in enumerate((p0, p1, p2, p3)):
        p = params[16 + m]
        n_rows = params[4 + m]
        n_cols = params[8 + m]
        both = n_rows.astype(jnp.float32) + n_cols.astype(jnp.float32)
        norm = -jnp.log(jnp.full((1, 128), both))
        line = pay[pl.ds(mine, 1), :]
        pot = jnp.transpose(jnp.broadcast_to(line, (BLK, 128)))
        row_kept = mine * BLK + row_id < n_rows
        line = jnp.where(mine * BLK + lanes < n_rows, alpha + line + pay[33:34, :] - norm, 0.0)
        side = jnp.where(quarter == p, line, side)
        for c in range(NCH):
            spot = pl.ds(c * 128, 128)
            col_pot = pay[NBLK + c : NBLK + c + 1, :]
            col_kept = c * 128 + lanes < n_cols
            tile = scores[m, :, spot] + pot + col_pot - norm
            block[m, :, spot] = jnp.where(row_kept & col_kept, tile, 0.0)
            line = jnp.where(col_kept, alpha + pay[32:33, :] + col_pot - norm, 0.0)
            edges[c] = jnp.where(quarter == p, line, edges[c])
            if c % 8 == 7:
                half = pl.ds((c // 8) * (KP // 2), KP // 2)
                copy = pltpu.make_async_copy(
                    block.at[m, :, half], match.at[p, :, half], sems.at[m, c // 8]
                )
                copy.start()
                stores.append(copy)
    row_bins[...] = side
    for c in range(NCH):
        col_bins[:, pl.ds(c * 128, 128)] = edges[c]
    for copy in stores:
        copy.wait()


SMEM = functools.partial(pl.BlockSpec, memory_space=pltpu.SMEM)
VMEM = functools.partial(pl.BlockSpec, memory_space=pltpu.VMEM)
ANY = functools.partial(pl.BlockSpec, memory_space=pl.ANY)


def run_sinkhorn(params, bins, xs):
    f32 = jnp.float32
    return pl.pallas_call(
        sinkhorn_kernel,
        out_shape=jax.ShapeDtypeStruct((40, 128), f32),
        in_specs=[SMEM()] * 2 + [ANY()] * 4,
        out_specs=VMEM(),
        scratch_shapes=[
            pltpu.VMEM((KP, KP), f32),
            pltpu.VMEM((BIG, KP), f32),
            pltpu.VMEM((BIG, KP), f32),
            pltpu.VMEM((KP, D), jnp.bfloat16),
            pltpu.VMEM((KP, D), jnp.bfloat16),
            pltpu.VMEM((2 * BIG, 128), f32),
            pltpu.VMEM((KP, 128), f32),
            pltpu.VMEM((KP, 128), f32),
            pltpu.VMEM((KP, 128), f32),
            pltpu.VMEM((KP, 128), f32),
            pltpu.VMEM((8, KP), f32),
            pltpu.VMEM((8, KP), f32),
            pltpu.SemaphoreType.DMA((4, 4, 2)),
        ],
        compiler_params=pltpu.CompilerParams(vmem_limit_bytes=40 * 1024 * 1024),
        cost_estimate=pl.CostEstimate(
            flops=200_000_000_000, bytes_accessed=2 << 20, transcendentals=0
        ),
        name="sinkhorn",
    )(params, bins, *xs)


def run_pick(index, desc):
    part = jax.ShapeDtypeStruct((2, BLK, D), jnp.bfloat16)
    more = jax.ShapeDtypeStruct((3, BLK, D), jnp.bfloat16)
    return pl.pallas_call(
        pick_kernel,
        out_shape=(part,) * 4 + (more,) * 4 + (jax.ShapeDtypeStruct((20,), jnp.int32),),
        in_specs=[SMEM(), ANY()],
        out_specs=[VMEM()] * 8 + [SMEM()],
        scratch_shapes=[pltpu.SemaphoreType.DMA((4, 2)), pltpu.SemaphoreType.DMA((4, 3))],
        compiler_params=pltpu.CompilerParams(vmem_limit_bytes=6 * 1024 * 1024),
        name="pick",
    )(index, desc)


def run_scores(params, desc, xs, ys):
    return pl.pallas_call(
        score_kernel,
        out_shape=jax.ShapeDtypeStruct((4, BLK, KP), jnp.float32),
        in_specs=[SMEM(), VMEM()] + [ANY()] * 8,
        out_specs=VMEM(),
        scratch_shapes=[
            pltpu.VMEM((4, 4, BLK, D), jnp.bfloat16),
            pltpu.VMEM((4, 4, 3, BLK, D), jnp.bfloat16),
            pltpu.SemaphoreType.DMA((2, 4)),
        ],
        compiler_params=pltpu.CompilerParams(vmem_limit_bytes=16 * 1024 * 1024),
        cost_estimate=pl.CostEstimate(
            flops=8_000_000_000, bytes_accessed=8 << 20, transcendentals=0
        ),
        name="scores",
    )(params, desc, *xs, *ys)


def run_finish(params, bins, scores, pays):
    f32 = jnp.float32
    return pl.pallas_call(
        finish_kernel,
        out_shape=(
            jax.ShapeDtypeStruct((4, BLK, KP), f32),
            jax.ShapeDtypeStruct((4, BLK), f32),
            jax.ShapeDtypeStruct((4, KP), f32),
        ),
        in_specs=[SMEM()] * 2 + [VMEM()] * 5,
        out_specs=(ANY(), VMEM(), VMEM()),
        scratch_shapes=[pltpu.VMEM((4, BLK, KP), f32), pltpu.SemaphoreType.DMA((4, 2))],
        compiler_params=pltpu.CompilerParams(vmem_limit_bytes=16 * 1024 * 1024),
        name="finish",
    )(params, bins, scores, *pays)


def shifts(groups, along_b):
    def perm(k):
        moves = []
        for g in range(groups):
            for i in range(4):
                for j in range(4):
                    on_row_1 = (g % 2 == 0) == along_b
                    to = (i, (j + k) % 4) if on_row_1 else ((i + k) % 4, j)
                    moves.append((g * 16 + i * 4 + j, g * 16 + to[0] * 4 + to[1]))
        return moves

    return perm


def on_device(descriptors, counts, pairs, bin_score):
    groups = lax.axis_size("pair")
    even = lax.axis_index("pair") % 2 == 0
    i, j = lax.axis_index("row_0"), lax.axis_index("row_1")
    a, b = jnp.where(even, i, j), jnp.where(even, j, i)
    by_b, by_a = shifts(groups, True), shifts(groups, False)

    index = jnp.stack([a, b, even.astype(jnp.int32), i * 4 + j]).astype(jnp.int32)
    index = jnp.concatenate([index, counts, pairs.reshape(-1)])
    s0, s1, s2, s3, e0, e1, e2, e3, params = run_pick(index, descriptors)

    def send(parts, moves):
        arrived = []
        for k, x in enumerate(parts, 1):
            arrived.append(lax.ppermute(x, AXES, moves(k)))
        return arrived

    x0 = jnp.stack([s0] + send((s1, s2, s3), by_b))
    xs = [x0] + send((x0, x0, x0), by_a)
    y0 = jnp.stack([e0] + send((e1, e2, e3), by_b))
    ys = [y0] + send((y0, y0, y0), by_a)
    pay = run_sinkhorn(params, bin_score, xs)
    pays = [pay] + [lax.ppermute(pay, AXES, by_b(k)) for k in (1, 2, 3)]
    desc, late = lax.optimization_barrier((descriptors, pay))
    scores = run_scores(params, desc, xs, ys)
    return run_finish(params, bin_score, scores, [late] + pays[1:])


def solution(mesh):
    finer = Mesh(mesh.devices.reshape(mesh.shape["pair"], 4, 4), AXES)
    rows = ("row_0", "row_1")
    in_specs = (P("pair", rows, None), P("pair"), P("pair", None), P())
    out_specs = (P("pair", rows, None), P("pair", rows), P("pair", None))
    return jax.shard_map(
        on_device, mesh=finer, in_specs=in_specs, out_specs=out_specs, check_vma=False
    )
```
